8 devices in a mesh: dp: 1 (over z), tp: 8 (over y, x, core).
Axes of the slice: x: 2, y: 2, z: 1, core: 2. Of those that a mesh axis runs over, the one named last changes fastest.
Arguments:
- hidden: bfloat16 [1, 8192, 4096], P('dp', 'tp')
- attn_gain: float32 [4096], replicated
- attn_bias: float32 [4096], replicated
- mlp_gain: float32 [4096], replicated
- mlp_bias: float32 [4096], replicated
- w_qkv: bfloat16 [4096, 8, 768], P(None, 'tp')
- w_out: bfloat16 [4096, 4096], P('tp')
- w_up: bfloat16 [4096, 16384], P(None, 'tp')
- w_down: bfloat16 [16384, 4096], P('tp')
- positions: int32 [8192], replicated
Outputs:
- output: bfloat16 [1, 8192, 4096], P('dp', 'tp')
All inputs are finite; a program needn't handle non-finite values.
Results may differ from the reference program's by a relative error of at most 0.00473784.
Values are sent between devices in bfloat16 or wider.
A program may use at most 1 GiB of HBM per device.

```python
import jax
import jax.numpy as jnp
from jax import lax

D = 4096
HEADS = 32
KV_HEADS = 8
HEAD = 128
FF = 16384
BATCH = 1
SEQ_LEN = 8192
QUERY_BLOCK = 64
HALF_HEAD = 64

GROUP_SIZE = HEADS // KV_HEADS
QKV_COLS = (GROUP_SIZE + 2) * HEAD


def setup_inputs(seed: int = 0, part: int = 0) -> dict:
    root_key = jax.random.key(seed)
    sub_keys = jax.random.split(root_key, 10)
    part_key = jax.random.fold_in(sub_keys[0], part)
    hidden = jax.random.normal(part_key, (BATCH, SEQ_LEN, D), jnp.float32).astype(jnp.bfloat16)
    attn_gain = 1.0 + 0.4 * jax.random.normal(sub_keys[1], (D,), jnp.float32)
    attn_bias = 0.4 * jax.random.normal(sub_keys[2], (D,), jnp.float32)
    mlp_gain = 1.0 + 0.4 * jax.random.normal(sub_keys[3], (D,), jnp.float32)
    mlp_bias = 0.4 * jax.random.normal(sub_keys[4], (D,), jnp.float32)
    w_qkv = (1.2 * D ** -0.5 * jax.random.normal(sub_keys[5], (D, KV_HEADS, QKV_COLS), jnp.float32)).astype(jnp.bfloat16)
    w_out = (2.0 * (HEADS * HEAD) ** -0.5 * jax.random.normal(sub_keys[6], (HEADS * HEAD, D), jnp.float32)).astype(jnp.bfloat16)
    w_up = (D ** -0.5 * jax.random.normal(sub_keys[7], (D, FF), jnp.float32)).astype(jnp.bfloat16)
    w_down = (FF ** -0.5 * jax.random.normal(sub_keys[8], (FF, D), jnp.float32)).astype(jnp.bfloat16)
    pos_gaps = jax.random.randint(sub_keys[9], (SEQ_LEN,), 1, 4, jnp.int32)
    positions = (jnp.cumsum(pos_gaps) - pos_gaps[0]).astype(jnp.int32)
    return {'hidden': hidden, 'attn_gain': attn_gain, 'attn_bias': attn_bias, 'mlp_gain': mlp_gain, 'mlp_bias': mlp_bias, 'w_qkv': w_qkv, 'w_out': w_out, 'w_up': w_up, 'w_down': w_down, 'positions': positions}


def layer_norm(tok_rows, norm_gain, norm_bias):
    rows32 = tok_rows.astype(jnp.float32)
    row_mean = jnp.mean(rows32, axis=-1, keepdims=True)
    centered = rows32 - row_mean
    row_var = jnp.mean(centered * centered, axis=-1, keepdims=True)
    return (centered * lax.rsqrt(row_var + 1e-5) * norm_gain + norm_bias).astype(jnp.bfloat16)


def apply_rotary(head_vals, cos_tab, sin_tab):
    vals32 = head_vals.astype(jnp.float32)
    rotated = jnp.concatenate([-vals32[..., HALF_HEAD:], vals32[..., :HALF_HEAD]], axis=-1)
    return (vals32 * cos_tab + rotated * sin_tab).astype(jnp.bfloat16)


def attend_sequence(query_rot, key_rot, value_seq):
    key32 = key_rot.astype(jnp.float32)
    value32 = value_seq.astype(jnp.float32)
    key_idx = jnp.arange(SEQ_LEN)

    def one_block(block_idx):
        row_start = block_idx * QUERY_BLOCK
        query_blk = lax.dynamic_slice_in_dim(query_rot, row_start, QUERY_BLOCK, axis=0).astype(jnp.float32)
        scores = jnp.einsum('qkgh,skh->kgqs', query_blk, key32) * HEAD ** -0.5
        query_idx = row_start + jnp.arange(QUERY_BLOCK)
        allowed = key_idx[None, :] <= query_idx[:, None]
        scores = jnp.where(allowed, scores, -1e30)
        exp_scores = jnp.exp(scores - jnp.max(scores, axis=-1, keepdims=True))
        attn_probs = (exp_scores / jnp.sum(exp_scores, axis=-1, keepdims=True)).astype(jnp.bfloat16)
        context = jnp.einsum('kgqs,skh->qkgh', attn_probs.astype(jnp.float32), value32)
        return context.astype(jnp.bfloat16)

    ctx_blocks = lax.map(one_block, jnp.arange(SEQ_LEN // QUERY_BLOCK))
    return ctx_blocks.reshape(SEQ_LEN, HEADS * HEAD)


def reference(hidden, attn_gain, attn_bias, mlp_gain, mlp_bias, w_qkv, w_out, w_up, w_down, positions):
    inv_freq = 10000.0 ** (-2.0 * jnp.arange(HALF_HEAD, dtype=jnp.float32) / HEAD)
    angles = positions.astype(jnp.float32)[:, None] * inv_freq[None, :]
    angles = jnp.concatenate([angles, angles], axis=-1)
    cos_tab = jnp.cos(angles)
    sin_tab = jnp.sin(angles)
    w_qkv_flat = w_qkv.reshape(D, KV_HEADS * QKV_COLS)

    def one_sequence(seq_rows):
        normed_attn = layer_norm(seq_rows, attn_gain, attn_bias)
        normed_mlp = layer_norm(seq_rows, mlp_gain, mlp_bias)
        qkv_rows = jnp.dot(normed_attn, w_qkv_flat, preferred_element_type=jnp.float32).astype(jnp.bfloat16)
        qkv_rows = qkv_rows.reshape(SEQ_LEN, KV_HEADS, GROUP_SIZE + 2, HEAD)
        query_rot = apply_rotary(qkv_rows[:, :, :GROUP_SIZE, :], cos_tab[:, None, None, :], sin_tab[:, None, None, :])
        key_rot = apply_rotary(qkv_rows[:, :, GROUP_SIZE, :], cos_tab[:, None, :], sin_tab[:, None, :])
        value_seq = qkv_rows[:, :, GROUP_SIZE + 1, :]
        context = attend_sequence(query_rot, key_rot, value_seq)
        attn_part = jnp.dot(context, w_out, preferred_element_type=jnp.float32)
        up_pre = jnp.dot(normed_mlp, w_up, preferred_element_type=jnp.float32)
        up_act = jax.nn.gelu(up_pre, approximate=False).astype(jnp.bfloat16)
        mlp_part = jnp.dot(up_act, w_down, preferred_element_type=jnp.float32)
        return (seq_rows.astype(jnp.float32) + attn_part + mlp_part).astype(jnp.bfloat16)

    return lax.map(one_sequence, hidden)
```

```python
import functools

import jax
import jax.numpy as jnp
from jax import lax
from jax.experimental import pallas as pl
from jax.experimental.pallas import tpu as pltpu
from jax.sharding import PartitionSpec as P


CHUNKS = 4
KV_BLOCK = 512
HEAD = 128
LOG2E = 1.4426950408889634
NORM_ROWS = 16
TILE = 256


def norm_kernel(core_ref, x_ref, ag_ref, ab_ref, mg_ref, mb_ref, a_ref, m_ref):
    width = x_ref.shape[-1]

    def group(i, carry):
        rows = pl.ds(pl.multiple_of(i * NORM_ROWS, NORM_ROWS), NORM_ROWS)
        tiles = [x_ref[rows, t * 512:(t + 1) * 512].astype(jnp.float32) for t in range(width // 512)]
        mean = jnp.sum(functools.reduce(jnp.add, tiles), axis=-1, keepdims=True) * (1.0 / width)
        tiles = [tile - mean for tile in tiles]
        var = jnp.sum(functools.reduce(jnp.add, [tile * tile for tile in tiles]), axis=-1, keepdims=True) * (1.0 / width)
        inv = lax.rsqrt(var + 1e-5)
        for t, tile in enumerate(tiles):
            cols = slice(t * 512, (t + 1) * 512)
            unit = tile * inv
            a_ref[rows, cols] = (unit * ag_ref[:, cols] + ab_ref[:, cols]).astype(jnp.bfloat16)
            m_ref[rows, cols] = (unit * mg_ref[:, cols] + mb_ref[:, cols]).astype(jnp.bfloat16)
        return carry

    lax.fori_loop(0, x_ref.shape[0] // NORM_ROWS, group, 0, unroll=2)


def two_norms(core, rows, blk, attn_gain, attn_bias, mlp_gain, mlp_bias):
    num_rows, width = rows.shape
    sub = min(blk, 256)
    per = blk // sub
    chips = num_rows // (2 * blk)

    def source(i, core_ref):
        half = i // (chips * per)
        chip = (i // per) % chips
        dev = 2 * chip + jnp.where(half == 0, 1 - core_ref[0], core_ref[0])
        return (dev * per + i % per, 0)

    vec = pl.BlockSpec((1, width), lambda i, core_ref: (0, 0))
    out = pl.BlockSpec((sub, width), lambda i, core_ref: (i, 0))
    return pl.pallas_call(
        norm_kernel,
        grid_spec=pltpu.PrefetchScalarGridSpec(
            num_scalar_prefetch=1,
            grid=(num_rows // sub,),
            in_specs=[pl.BlockSpec((sub, width), source), vec, vec, vec, vec],
            out_specs=[out, out],
        ),
        out_shape=[jax.ShapeDtypeStruct((num_rows, width), jnp.bfloat16)] * 2,
        cost_estimate=pl.CostEstimate(flops=num_rows * width * 500, bytes_accessed=num_rows * width * 6, transcendentals=0),
        name="two_norms",
    )(core, rows, attn_gain[None], attn_bias[None], mlp_gain[None], mlp_bias[None])


def rotate_kernel(x_ref, cos_ref, sin_ref, q_ref, k_ref):
    cos_tab, sin_tab = cos_ref[...], sin_ref[...]
    q_heads = q_ref.shape[1] // HEAD
    for h in range(q_heads + 1):
        vals32 = x_ref[:, h * HEAD:(h + 1) * HEAD].astype(jnp.float32)
        turned = (vals32 * cos_tab + pltpu.roll(vals32, HEAD // 2, 1) * sin_tab).astype(jnp.bfloat16)
        if h < q_heads:
            q_ref[:, h * HEAD:(h + 1) * HEAD] = turned
        else:
            k_ref[...] = turned


def rotate(qkv, cos_tab, sin_tab):
    num_rows, cols = qkv.shape
    q_cols = cols - 2 * HEAD
    sub = min(num_rows, 256)

    def spec(c):
        return pl.BlockSpec((sub, c), lambda i: (i, 0))

    return pl.pallas_call(
        rotate_kernel,
        grid=(num_rows // sub,),
        in_specs=[spec(cols), spec(HEAD), spec(HEAD)],
        out_specs=[spec(q_cols), spec(HEAD)],
        out_shape=[jax.ShapeDtypeStruct((num_rows, q_cols), jnp.bfloat16), jax.ShapeDtypeStruct((num_rows, HEAD), jnp.bfloat16)],
        cost_estimate=pl.CostEstimate(flops=num_rows * cols * 500, bytes_accessed=num_rows * cols * 5, transcendentals=0),
        name="rotate",
    )(qkv, cos_tab, sin_tab)


def up_gelu_kernel(x_ref, w_ref, o_ref):
    spots = [(r, c) for c in range(0, o_ref.shape[1], TILE) for r in range(0, o_ref.shape[0], TILE)]

    def pre(r, c):
        return jnp.dot(x_ref[r:r + TILE, :], w_ref[:, c:c + TILE], preferred_element_type=jnp.float32)

    held = pre(*spots[0])
    for n, (r, c) in enumerate(spots):
        ahead = pre(*spots[n + 1]) if n + 1 < len(spots) else None
        o_ref[r:r + TILE, c:c + TILE] = (0.5 * held * (1.0 + lax.erf(held * 0.7071067811865476))).astype(jnp.bfloat16)
        held = ahead


def up_gelu(rows, w_up):
    num_rows, width = rows.shape
    cols = w_up.shape[1]
    sub, wide = min(num_rows, 1024), min(cols, 512)
    return pl.pallas_call(
        up_gelu_kernel,
        grid=(num_rows // sub, cols // wide),
        in_specs=[pl.BlockSpec((sub, width), lambda i, j: (i, 0)), pl.BlockSpec((width, wide), lambda i, j: (0, j))],
        out_specs=pl.BlockSpec((sub, wide), lambda i, j: (i, j)),
        out_shape=jax.ShapeDtypeStruct((num_rows, cols), jnp.bfloat16),
        cost_estimate=pl.CostEstimate(flops=2 * num_rows * width * cols, bytes_accessed=2 * num_rows * (width + cols) + 4 * width * cols, transcendentals=0),
        name="up_gelu",
    )(rows, w_up)


def project_kernel(ctx_ref, up_ref, wo_ref, wd_ref, *rest):
    o_ref = rest[-1]
    for c in range(0, o_ref.shape[1], TILE):
        for r in range(0, o_ref.shape[0], TILE):
            total = jnp.dot(ctx_ref[r:r + TILE, :], wo_ref[:, c:c + TILE], preferred_element_type=jnp.float32)
            total += jnp.dot(up_ref[r:r + TILE, :], wd_ref[:, c:c + TILE], preferred_element_type=jnp.float32)
            if len(rest) == 2:
                total += rest[0][r:r + TILE, c:c + TILE].astype(jnp.float32)
            o_ref[r:r + TILE, c:c + TILE] = total.astype(o_ref.dtype)


def project(context, up_rows, w_out, w_down, half, num_rows, part, parts, take, dtype):
    cols = w_out.shape[1] // parts
    wide = min(cols, 512)
    first = part * (cols // wide)
    depth = w_out.shape[0] + w_down.shape[0]
    in_specs = [
        pl.BlockSpec((num_rows, context.shape[1]), lambda j: (half, 0)),
        pl.BlockSpec((num_rows, up_rows.shape[1]), lambda j: (half, 0)),
        pl.BlockSpec((w_out.shape[0], wide), lambda j: (0, first + j)),
        pl.BlockSpec((w_down.shape[0], wide), lambda j: (0, first + j)),
    ]
    args = [context, up_rows, w_out, w_down]
    out_spec = pl.BlockSpec((num_rows, wide), lambda j: (0, j))
    if take is not None:
        in_specs.append(out_spec)
        args.append(take)
    return pl.pallas_call(
        project_kernel,
        grid=(cols // wide,),
        in_specs=in_specs,
        out_specs=out_spec,
        out_shape=jax.ShapeDtypeStruct((num_rows, cols), dtype),
        cost_estimate=pl.CostEstimate(flops=2 * num_rows * depth * cols, bytes_accessed=2 * depth * (num_rows + cols) + 4 * num_rows * cols, transcendentals=0),
        name="project",
    )(*args)


def attend_kernel(group, q_blk, seg, offset, chips, core_ref, q_ref, k_ref, v_ref, o_ref, m_ref, l_ref, acc_ref):
    i = pl.program_id(0)
    half = i // chips
    dev = 2 * (i % chips) + jnp.where(half == 0, 1 - core_ref[0], core_ref[0])
    row_start = dev * seg + offset
    scale = HEAD ** -0.5 * LOG2E
    m_ref[...] = jnp.full(m_ref.shape, -1e30, jnp.float32)
    l_ref[...] = jnp.zeros(l_ref.shape, jnp.float32)
    acc_ref[...] = jnp.zeros(acc_ref.shape, jnp.float32)
    lanes = KV_BLOCK // HEAD

    def block(col_start, masked):
        cols = pl.ds(pl.multiple_of(col_start, KV_BLOCK), KV_BLOCK)
        key_blk = k_ref[cols, :]
        value_blk = v_ref[cols, :]
        if masked:
            row_idx = row_start + lax.broadcasted_iota(jnp.int32, (q_blk, KV_BLOCK), 0)
            col_idx = col_start + lax.broadcasted_iota(jnp.int32, (q_blk, KV_BLOCK), 1)
            allowed = col_idx <= row_idx

        def score(h):
            query = q_ref[:, h * HEAD:(h + 1) * HEAD]
            scores = lax.dot_general(query, key_blk, (((1,), (1,)), ((), ())), preferred_element_type=jnp.float32)
            return jnp.where(allowed, scores, -1e30) if masked else scores

        def weigh(h, scores):
            m_prev = m_ref[h]
            m_next = jnp.maximum(m_prev, jnp.max(scores, axis=1, keepdims=True))
            m_ref[h] = m_next
            alpha = jnp.exp2((m_prev - m_next) * scale)
            probs = [jnp.exp2((scores[:, t * HEAD:(t + 1) * HEAD] - m_next) * scale) for t in range(lanes)]
            l_ref[h] = alpha * l_ref[h] + functools.reduce(jnp.add, probs)
            return alpha, jnp.concatenate([p.astype(jnp.bfloat16) for p in probs], axis=1)

        def gather_values(h, alpha, prob_blk):
            acc_ref[h] = alpha * acc_ref[h] + jnp.dot(prob_blk, value_blk, preferred_element_type=jnp.float32)

        scores = score(0)
        held = None
        for h in range(group):
            ahead = score(h + 1) if h + 1 < group else None
            now = weigh(h, scores)
            if held is not None:
                gather_values(h - 1, *held)
            held, scores = now, ahead
        gather_values(group - 1, *held)

    full = row_start // KV_BLOCK

    def step(j, carry):
        block(j * KV_BLOCK, False)
        return carry

    lax.fori_loop(0, full, step, 0)
    block(full * KV_BLOCK, True)
    for h in range(group):
        total = jnp.sum(l_ref[h], axis=1, keepdims=True)
        o_ref[:, h * HEAD:(h + 1) * HEAD] = (acc_ref[h] / total).astype(jnp.bfloat16)


def attend(core, q_rows, keys, values, q_blk, seg, offset):
    num_rows, q_cols = q_rows.shape
    seq_len = keys.shape[0]
    group = q_cols // HEAD
    chips = num_rows // (2 * q_blk)
    row_spec = pl.BlockSpec((q_blk, q_cols), lambda i, core_ref: (i, 0))
    kv_spec = pl.BlockSpec((seq_len, HEAD), lambda i, core_ref: (0, 0))
    stat = pltpu.VMEM((group, q_blk, HEAD), jnp.float32)
    return pl.pallas_call(
        functools.partial(attend_kernel, group, q_blk, seg, offset, chips),
        grid_spec=pltpu.PrefetchScalarGridSpec(
            num_scalar_prefetch=1,
            grid=(num_rows // q_blk,),
            in_specs=[row_spec, kv_spec, kv_spec],
            out_specs=row_spec,
            scratch_shapes=[stat, stat, stat],
        ),
        out_shape=jax.ShapeDtypeStruct((num_rows, q_cols), jnp.bfloat16),
        cost_estimate=pl.CostEstimate(
            flops=num_rows * seq_len * q_cols * 8, bytes_accessed=num_rows * q_cols * 4 + seq_len * HEAD * 4, transcendentals=num_rows * seq_len * group // 2
        ),
        name="attend",
    )(core, q_rows, keys, values)


def rotary_tables(positions):
    inv_freq = 10000.0 ** (-2.0 * jnp.arange(HEAD // 2, dtype=jnp.float32) / HEAD)
    angles = positions.astype(jnp.float32)[:, None] * inv_freq[None, :]
    cos_half, sin_half = jnp.cos(angles), jnp.sin(angles)
    return jnp.concatenate([cos_half, cos_half], axis=-1), jnp.concatenate([-sin_half, sin_half], axis=-1)


def solution(mesh):
    tp = mesh.shape['tp']
    chips = tp // 2

    def swap(bits):
        return [(d, d ^ bits) for d in range(tp)]

    def dot32(left, right):
        return jnp.dot(left, right, preferred_element_type=jnp.float32)

    def local_layer(hidden_blk, attn_gain, attn_bias, mlp_gain, mlp_bias, w_qkv_part, w_out_part, w_up_part, w_down_part, positions):
        me = lax.axis_index('tp')
        core_bit = me % 2
        chip = me // 2
        core = core_bit.astype(jnp.int32)[None]
        seg, width = hidden_blk.shape[1:]
        blk = seg // CHUNKS
        x_rows = hidden_blk[0]
        w_qkv_flat = w_qkv_part[:, 0, :]
        group_cols = w_out_part.shape[0]

        cos_tab, sin_tab = rotary_tables(positions)

        def own_order(table):
            table = table.reshape(chips, 2, CHUNKS, blk, HEAD)
            table = jnp.where(core_bit == 0, table[:, ::-1], table)
            return table.transpose(2, 1, 0, 3, 4).reshape(CHUNKS, tp * blk, HEAD)

        cos_own, sin_own = own_order(cos_tab), own_order(sin_tab)

        gathered = [lax.all_gather(x_rows[c * blk:(c + 1) * blk], 'tp', axis=0, tiled=True) for c in range(CHUNKS)]
        queries, keys, values, ups = [], [], [], []
        prev = None
        for c in range(CHUNKS):
            rows = gathered[c]
            if prev is not None:
                rows, ups[-1] = lax.optimization_barrier((rows, prev))
            normed_attn, normed_mlp = two_norms(core, rows, blk, attn_gain, attn_bias, mlp_gain, mlp_bias)
            qkv = dot32(normed_attn, w_qkv_flat).astype(jnp.bfloat16)
            query, key = rotate(qkv, cos_own[c], sin_own[c])
            queries.append(query)
            keys.append(key)
            values.append(qkv[:, group_cols + HEAD:])
            prev = up_gelu(normed_mlp, w_up_part)
            ups.append(prev)

        def device_major(parts):
            stacked = jnp.stack(parts).reshape(CHUNKS, 2, chips, blk, HEAD)
            stacked = jnp.where(core_bit == 0, stacked[:, ::-1], stacked)
            return stacked.transpose(2, 1, 0, 3, 4).reshape(tp * seg, HEAD)

        all_keys, all_values = device_major(keys), device_major(values)

        half = chips * blk

        def partner(give):
            return lax.ppermute(give, 'tp', swap(1))

        def split(keep, c, cols):
            pair = keep.reshape(chips, blk, keep.shape[1])
            own = x_rows[c * blk:(c + 1) * blk, cols].astype(jnp.float32) + lax.dynamic_index_in_dim(pair, chip, 0, keepdims=False)
            return own, [lax.dynamic_index_in_dim(pair, chip ^ flip, 0, keepdims=False).astype(jnp.bfloat16) for flip in range(1, chips)]

        def send(own, away):
            for flip, block in zip(range(1, chips), away):
                moved = lax.ppermute(block, 'tp', swap(2 * flip))
                own = own + moved.astype(jnp.float32)
            return own.astype(jnp.bfloat16)

        def attended(c):
            return attend(core, queries[c], all_keys, all_values, blk, seg, c * blk)

        def give_rows(context, c, part, parts):
            return project(context, ups[c], w_out_part, w_down_part, 0, half, part, parts, None, jnp.bfloat16)

        def keep_rows(context, c, part, parts, take):
            return project(context, ups[c], w_out_part, w_down_part, 1, half, part, parts, take, jnp.float32)

        outs = []
        every = slice(0, width)
        ready = None
        for c in range(CHUNKS - 1):
            context = attended(c)
            if ready is not None:
                outs.append(send(*ready))
            give = give_rows(context, c, 0, 1)
            if c > 0:
                queries[c + 1], give = lax.optimization_barrier((queries[c + 1], give))
            ready = split(keep_rows(context, c, 0, 1, partner(give)), c, every)
            if c == 0:
                queries[1], ready = lax.optimization_barrier((queries[1], ready))
        c = CHUNKS - 1
        context = attended(c)
        outs.append(send(*ready))
        takes = [partner(give_rows(context, c, part, 2)) for part in range(2)]
        tails = []
        for part in range(2):
            cols = slice(part * (width // 2), (part + 1) * (width // 2))
            ready = split(keep_rows(context, c, part, 2, takes[part]), c, cols)
            if part == 0:
                ready, takes[1] = lax.optimization_barrier((ready, takes[1]))
            tails.append(send(*ready))
        outs.append(jnp.concatenate(tails, axis=1))
        return jnp.concatenate(outs)[None]

    return jax.shard_map(local_layer, mesh=mesh, in_specs=(P('dp', 'tp', None), P(), P(), P(), P(), P(None, 'tp', None), P('tp', None), P(None, 'tp'), P('tp', None), P()), out_specs=P('dp', 'tp', None), check_vma=False)
```

```python
import functools

import jax
import jax.numpy as jnp
from jax import lax
from jax.experimental import pallas as pl
from jax.experimental.pallas import tpu as pltpu
from jax.sharding import PartitionSpec as P


SHARES = (1, 1, 1, 1)
KV_BLOCK = 512
Q_ALIGN = 128
HEAD = 128
LOG2E = 1.4426950408889634
NORM_ROWS = 16
TILE = 256


def norm_kernel(core_ref, x_ref, ag_ref, ab_ref, mg_ref, mb_ref, a_ref, m_ref):
    width = x_ref.shape[-1]

    def group(i, carry):
        rows = pl.ds(pl.multiple_of(i * NORM_ROWS, NORM_ROWS), NORM_ROWS)
        tiles = [x_ref[rows, t * 512:(t + 1) * 512].astype(jnp.float32) for t in range(width // 512)]
        mean = jnp.sum(functools.reduce(jnp.add, tiles), axis=-1, keepdims=True) * (1.0 / width)
        tiles = [tile - mean for tile in tiles]
        var = jnp.sum(functools.reduce(jnp.add, [tile * tile for tile in tiles]), axis=-1, keepdims=True) * (1.0 / width)
        inv = lax.rsqrt(var + 1e-5)
        for t, tile in enumerate(tiles):
            cols = slice(t * 512, (t + 1) * 512)
            unit = tile * inv
            a_ref[rows, cols] = (unit * ag_ref[:, cols] + ab_ref[:, cols]).astype(jnp.bfloat16)
            m_ref[rows, cols] = (unit * mg_ref[:, cols] + mb_ref[:, cols]).astype(jnp.bfloat16)
        return carry

    lax.fori_loop(0, x_ref.shape[0] // NORM_ROWS, group, 0, unroll=2)


def two_norms(core, rows, blk, attn_gain, attn_bias, mlp_gain, mlp_bias):
    num_rows, width = rows.shape
    sub = min(blk, 256)
    per = blk // sub
    chips = num_rows // (2 * blk)

    def source(i, core_ref):
        half = i // (chips * per)
        chip = (i // per) % chips
        dev = 2 * chip + jnp.where(half == 0, 1 - core_ref[0], core_ref[0])
        return (dev * per + i % per, 0)

    vec = pl.BlockSpec((1, width), lambda i, core_ref: (0, 0))
    out = pl.BlockSpec((sub, width), lambda i, core_ref: (i, 0))
    return pl.pallas_call(
        norm_kernel,
        grid_spec=pltpu.PrefetchScalarGridSpec(
            num_scalar_prefetch=1,
            grid=(num_rows // sub,),
            in_specs=[pl.BlockSpec((sub, width), source), vec, vec, vec, vec],
            out_specs=[out, out],
        ),
        out_shape=[jax.ShapeDtypeStruct((num_rows, width), jnp.bfloat16)] * 2,
        cost_estimate=pl.CostEstimate(flops=num_rows * width * 500, bytes_accessed=num_rows * width * 6, transcendentals=0),
        name="two_norms",
    )(core, rows, attn_gain[None], attn_bias[None], mlp_gain[None], mlp_bias[None])


def qkv_kernel(x_ref, w_ref, cos_ref, sin_ref, q_ref, k_ref, v_ref):
    num_rows, q_cols = q_ref.shape
    spots = [(r, c) for r in range(0, num_rows, TILE) for c in range(0, w_ref.shape[1], TILE)]

    def product(r, c):
        return jnp.dot(x_ref[r:r + TILE, :], w_ref[:, c:c + TILE], preferred_element_type=jnp.float32)

    held = product(*spots[0])
    for n, (r, c) in enumerate(spots):
        ahead = product(*spots[n + 1]) if n + 1 < len(spots) else None
        rows = slice(r, r + TILE)
        for start in range(0, TILE, HEAD):
            head = held[:, start:start + HEAD].astype(jnp.bfloat16)
            col = c + start
            if col == q_cols + HEAD:
                v_ref[rows, :] = head
                continue
            vals32 = head.astype(jnp.float32)
            turned = (vals32 * cos_ref[rows, :] + pltpu.roll(vals32, HEAD // 2, 1) * sin_ref[rows, :]).astype(jnp.bfloat16)
            if col == q_cols:
                k_ref[rows, :] = turned
            else:
                q_ref[rows, col:col + HEAD] = turned
        held = ahead


def project_qkv(rows, w_qkv, cos_tab, sin_tab):
    num_rows, width = rows.shape
    cols = w_qkv.shape[1]
    q_cols = cols - 2 * HEAD
    sub = min(num_rows, 512)

    def spec(c):
        return pl.BlockSpec((sub, c), lambda i: (i, 0))

    return pl.pallas_call(
        qkv_kernel,
        grid=(num_rows // sub,),
        in_specs=[spec(width), pl.BlockSpec((width, cols), lambda i: (0, 0)), spec(HEAD), spec(HEAD)],
        out_specs=[spec(q_cols), spec(HEAD), spec(HEAD)],
        out_shape=[jax.ShapeDtypeStruct((num_rows, c), jnp.bfloat16) for c in (q_cols, HEAD, HEAD)],
        cost_estimate=pl.CostEstimate(flops=2 * num_rows * width * cols, bytes_accessed=2 * num_rows * (width + cols) + 2 * width * cols, transcendentals=0),
        name="project_qkv",
    )(rows, w_qkv, cos_tab, sin_tab)


def up_gelu_kernel(x_ref, w_ref, o_ref):
    spots = [(r, c) for c in range(0, o_ref.shape[1], TILE) for r in range(0, o_ref.shape[0], TILE)]

    def pre(r, c):
        return jnp.dot(x_ref[r:r + TILE, :], w_ref[:, c:c + TILE], preferred_element_type=jnp.float32)

    held = pre(*spots[0])
    for n, (r, c) in enumerate(spots):
        ahead = pre(*spots[n + 1]) if n + 1 < len(spots) else None
        o_ref[r:r + TILE, c:c + TILE] = (0.5 * held * (1.0 + lax.erf(held * 0.7071067811865476))).astype(jnp.bfloat16)
        held = ahead


def up_gelu(rows, w_up):
    num_rows, width = rows.shape
    cols = w_up.shape[1]
    sub, wide = min(num_rows, 1024), min(cols, 512)
    return pl.pallas_call(
        up_gelu_kernel,
        grid=(num_rows // sub, cols // wide),
        in_specs=[pl.BlockSpec((sub, width), lambda i, j: (i, 0)), pl.BlockSpec((width, wide), lambda i, j: (0, j))],
        out_specs=pl.BlockSpec((sub, wide), lambda i, j: (i, j)),
        out_shape=jax.ShapeDtypeStruct((num_rows, cols), jnp.bfloat16),
        cost_estimate=pl.CostEstimate(flops=2 * num_rows * width * cols, bytes_accessed=2 * num_rows * (width + cols) + 4 * width * cols, transcendentals=0),
        name="up_gelu",
    )(rows, w_up)


def project_kernel(ctx_ref, up_ref, wo_ref, wd_ref, *rest):
    o_ref = rest[-1]
    for c in range(0, o_ref.shape[1], TILE):
        for r in range(0, o_ref.shape[0], TILE):
            total = jnp.dot(ctx_ref[r:r + TILE, :], wo_ref[:, c:c + TILE], preferred_element_type=jnp.float32)
            total += jnp.dot(up_ref[r:r + TILE, :], wd_ref[:, c:c + TILE], preferred_element_type=jnp.float32)
            if len(rest) == 2:
                total += rest[0][r:r + TILE, c:c + TILE].astype(jnp.float32)
            o_ref[r:r + TILE, c:c + TILE] = total.astype(o_ref.dtype)


def project(context, up_rows, w_out, w_down, half, num_rows, part, parts, take, dtype):
    cols = w_out.shape[1] // parts
    wide = min(cols, 512)
    first = part * (cols // wide)
    depth = w_out.shape[0] + w_down.shape[0]
    in_specs = [
        pl.BlockSpec((num_rows, context.shape[1]), lambda j: (half, 0)),
        pl.BlockSpec((num_rows, up_rows.shape[1]), lambda j: (half, 0)),
        pl.BlockSpec((w_out.shape[0], wide), lambda j: (0, first + j)),
        pl.BlockSpec((w_down.shape[0], wide), lambda j: (0, first + j)),
    ]
    args = [context, up_rows, w_out, w_down]
    out_spec = pl.BlockSpec((num_rows, wide), lambda j: (0, j))
    if take is not None:
        in_specs.append(out_spec)
        args.append(take)
    return pl.pallas_call(
        project_kernel,
        grid=(cols // wide,),
        in_specs=in_specs,
        out_specs=out_spec,
        out_shape=jax.ShapeDtypeStruct((num_rows, cols), dtype),
        cost_estimate=pl.CostEstimate(flops=2 * num_rows * depth * cols, bytes_accessed=2 * depth * (num_rows + cols) + 4 * num_rows * cols, transcendentals=0),
        name="project",
    )(*args)


def attend_kernel(group, q_blk, seg, offset, chips, core_ref, q_ref, k_ref, v_ref, o_ref, m_ref, l_ref, acc_ref):
    i = pl.program_id(0)
    half = i // chips
    dev = 2 * (i % chips) + jnp.where(half == 0, 1 - core_ref[0], core_ref[0])
    row_start = dev * seg + offset
    scale = HEAD ** -0.5 * LOG2E
    m_ref[...] = jnp.full(m_ref.shape, -1e30, jnp.float32)
    l_ref[...] = jnp.zeros(l_ref.shape, jnp.float32)
    acc_ref[...] = jnp.zeros(acc_ref.shape, jnp.float32)

    def score(h, col_start, width, masked):
        cols = pl.ds(pl.multiple_of(col_start, Q_ALIGN), width)
        query = q_ref[:, h * HEAD:(h + 1) * HEAD]
        scores = lax.dot_general(query, k_ref[cols, :], (((1,), (1,)), ((), ())), preferred_element_type=jnp.float32)
        if masked:
            row_idx = row_start + lax.broadcasted_iota(jnp.int32, (q_blk, width), 0)
            col_idx = col_start + lax.broadcasted_iota(jnp.int32, (q_blk, width), 1)
            scores = jnp.where(col_idx <= row_idx, scores, -1e30)
        return scores

    def weigh(h, scores):
        m_prev = m_ref[h]
        m_next = jnp.maximum(m_prev, jnp.max(scores, axis=1, keepdims=True))
        m_ref[h] = m_next
        alpha = jnp.exp2((m_prev - m_next) * scale)
        probs = [jnp.exp2((scores[:, t:t + HEAD] - m_next) * scale) for t in range(0, scores.shape[1], HEAD)]
        l_ref[h] = alpha * l_ref[h] + functools.reduce(jnp.add, probs)
        return alpha, jnp.concatenate([p.astype(jnp.bfloat16) for p in probs], axis=1)

    def add_values(h, col_start, width, alpha, prob_blk):
        cols = pl.ds(pl.multiple_of(col_start, Q_ALIGN), width)
        acc_ref[h] = alpha * acc_ref[h] + jnp.dot(prob_blk, v_ref[cols, :], preferred_element_type=jnp.float32)

    def blocks(spans, masked):
        work = [(h,) + span for span in spans for h in range(group)]
        scores = score(*work[0], masked)
        held = None
        for n, unit in enumerate(work):
            ahead = score(*work[n + 1], masked) if n + 1 < len(work) else None
            now = weigh(unit[0], scores)
            if held is not None:
                add_values(*work[n - 1], *held)
            held, scores = now, ahead
        add_values(*work[-1], *held)

    full = row_start // KV_BLOCK

    def step(j, carry):
        blocks([(j * KV_BLOCK, KV_BLOCK)], False)
        return carry

    lax.fori_loop(0, full, step, 0)
    blocks([(full * KV_BLOCK, offset % KV_BLOCK + q_blk)], True)
    for h in range(group):
        total = jnp.sum(l_ref[h], axis=1, keepdims=True)
        o_ref[:, h * HEAD:(h + 1) * HEAD] = (acc_ref[h] / total).astype(jnp.bfloat16)


def attend(core, q_rows, keys, values, q_blk, seg, offset):
    num_rows, q_cols = q_rows.shape
    seq_len = keys.shape[0]
    group = q_cols // HEAD
    chips = num_rows // (2 * q_blk)
    row_spec = pl.BlockSpec((q_blk, q_cols), lambda i, core_ref: (i, 0))
    kv_spec = pl.BlockSpec((seq_len, HEAD), lambda i, core_ref: (0, 0))
    stat = pltpu.VMEM((group, q_blk, HEAD), jnp.float32)
    return pl.pallas_call(
        functools.partial(attend_kernel, group, q_blk, seg, offset, chips),
        grid_spec=pltpu.PrefetchScalarGridSpec(
            num_scalar_prefetch=1,
            grid=(num_rows // q_blk,),
            in_specs=[row_spec, kv_spec, kv_spec],
            out_specs=row_spec,
            scratch_shapes=[stat, stat, stat],
        ),
        out_shape=jax.ShapeDtypeStruct((num_rows, q_cols), jnp.bfloat16),
        cost_estimate=pl.CostEstimate(
            flops=num_rows * seq_len * q_cols * 8, bytes_accessed=num_rows * q_cols * 4 + seq_len * HEAD * 4, transcendentals=num_rows * seq_len * group // 2
        ),
        name="attend",
    )(core, q_rows, keys, values)


def rotary_tables(positions):
    inv_freq = 10000.0 ** (-2.0 * jnp.arange(HEAD // 2, dtype=jnp.float32) / HEAD)
    angles = positions.astype(jnp.float32)[:, None] * inv_freq[None, :]
    cos_half, sin_half = jnp.cos(angles), jnp.sin(angles)
    return jnp.concatenate([cos_half, cos_half], axis=-1), jnp.concatenate([-sin_half, sin_half], axis=-1)


def solution(mesh):
    tp = mesh.shape['tp']
    chips = tp // 2

    def swap(bits):
        return [(d, d ^ bits) for d in range(tp)]

    def local_layer(hidden_blk, attn_gain, attn_bias, mlp_gain, mlp_bias, w_qkv_part, w_out_part, w_up_part, w_down_part, positions):
        me = lax.axis_index('tp')
        core_bit = me % 2
        chip = me // 2
        core = core_bit.astype(jnp.int32)[None]
        seg, width = hidden_blk.shape[1:]
        sizes = [share * (seg // sum(SHARES)) for share in SHARES]
        starts = [sum(sizes[:c]) for c in range(len(sizes))]
        chunks = len(sizes)
        x_rows = hidden_blk[0]
        w_qkv_flat = w_qkv_part[:, 0, :]

        cos_tab, sin_tab = rotary_tables(positions)

        def own_order(table):
            table = table.reshape(chips, 2, seg, HEAD)
            table = jnp.where(core_bit == 0, table[:, ::-1], table).transpose(1, 0, 2, 3)
            return [table[:, :, start:start + size].reshape(tp * size, HEAD) for start, size in zip(starts, sizes)]

        cos_own, sin_own = own_order(cos_tab), own_order(sin_tab)

        gathered = [lax.all_gather(x_rows[start:start + size], 'tp', axis=0, tiled=True) for start, size in zip(starts, sizes)]
        queries, keys, values, ups = [], [], [], []
        prev = None
        for c in range(chunks):
            rows = gathered[c]
            if prev is not None:
                rows, ups[-1] = lax.optimization_barrier((rows, prev))
            normed_attn, normed_mlp = two_norms(core, rows, sizes[c], attn_gain, attn_bias, mlp_gain, mlp_bias)
            query, key, value = project_qkv(normed_attn, w_qkv_flat, cos_own[c], sin_own[c])
            queries.append(query)
            keys.append(key)
            values.append(value)
            prev = up_gelu(normed_mlp, w_up_part)
            ups.append(prev)

        def device_major(parts):
            parts = [part.reshape(2, chips, size, HEAD) for part, size in zip(parts, sizes)]
            joined = jnp.concatenate(parts, axis=2)
            joined = jnp.where(core_bit == 0, joined[::-1], joined)
            return joined.transpose(1, 0, 2, 3).reshape(tp * seg, HEAD)

        all_keys, all_values = device_major(keys), device_major(values)

        def partner(give):
            return lax.ppermute(give, 'tp', swap(1))

        def split(keep, c, cols):
            pair = keep.reshape(chips, sizes[c], keep.shape[1])
            own = x_rows[starts[c]:starts[c] + sizes[c], cols].astype(jnp.float32) + lax.dynamic_index_in_dim(pair, chip, 0, keepdims=False)
            return own, [lax.dynamic_index_in_dim(pair, chip ^ flip, 0, keepdims=False).astype(jnp.bfloat16) for flip in range(1, chips)]

        def send(own, away):
            for flip, block in zip(range(1, chips), away):
                moved = lax.ppermute(block, 'tp', swap(2 * flip))
                own = own + moved.astype(jnp.float32)
            return own.astype(jnp.bfloat16)

        def attended(c):
            return attend(core, queries[c], all_keys, all_values, sizes[c], seg, starts[c])

        def give_rows(context, c, part, parts):
            return project(context, ups[c], w_out_part, w_down_part, 0, chips * sizes[c], part, parts, None, jnp.bfloat16)

        def keep_rows(context, c, part, parts, take):
            return project(context, ups[c], w_out_part, w_down_part, 1, chips * sizes[c], part, parts, take, jnp.float32)

        every = slice(0, width)
        out = jnp.zeros((seg, width), jnp.bfloat16)
        ready = None
        for c in range(chunks - 1):
            context = attended(c)
            if ready is not None:
                out = lax.dynamic_update_slice(out, send(*ready), (starts[c - 1], 0))
            give = give_rows(context, c, 0, 1)
            early = c in (0, chunks - 2)
            if not early:
                queries[c + 1], give = lax.optimization_barrier((queries[c + 1], give))
            ready = split(keep_rows(context, c, 0, 1, partner(give)), c, every)
            if early:
                queries[c + 1], ready = lax.optimization_barrier((queries[c + 1], ready))
        c = chunks - 1
        context = attended(c)
        out = lax.dynamic_update_slice(out, send(*ready), (starts[c - 1], 0))
        takes = [partner(give_rows(context, c, part, 2)) for part in range(2)]
        for part in range(2):
            first = part * (width // 2)
            ready = split(keep_rows(context, c, part, 2, takes[part]), c, slice(first, first + width // 2))
            if part == 0:
                ready, takes[1] = lax.optimization_barrier((ready, takes[1]))
            out = lax.dynamic_update_slice(out, send(*ready), (starts[c], first))
        return out[None]


    return jax.shard_map(local_layer, mesh=mesh, in_specs=(P('dp', 'tp', None), P(), P(), P(), P(), P(None, 'tp', None), P('tp', None), P(None, 'tp'), P('tp', None), P()), out_specs=P('dp', 'tp', None), check_vma=False)
```
